128 devices in a mesh: seq: 4 (over x_lo, core), tensor: 32 (over z, y, x_hi).
Axes of the slice: x: 4 (x_hi: 2, x_lo: 2; x = x_hi * 2 + x_lo), y: 4, z: 4, core: 2. Of those that a mesh axis runs over, the one named last changes fastest.
Arguments:
- tokens: bfloat16 [2, 4096, 4096], P(None, 'seq', 'tensor'), may hold values from -6 to 6
- w_qkv: bfloat16 [4096, 3, 4096], P(None, None, 'tensor'), may hold values from -1 to 1
- q_gain: float32 [4096], P('tensor'), may hold values from 0.5 to 2.5
- k_gain: float32 [4096], P('tensor'), may hold values from 0.5 to 2.5
- w_out: bfloat16 [4096, 4096], P('tensor'), may hold values from -0.1875 to 0.1875
Outputs:
- mixed: bfloat16 [2, 4096, 4096], P(None, 'seq', 'tensor')
- peak: float32 [32], P('tensor')
- qk_scale: float32 [2, 2, 4096], P(None, None, 'seq')
The draws below stay inside these ranges and needn't reach their ends.
All inputs are finite; a program needn't handle non-finite values.
Results may differ from the reference program's by a relative error of at most 0.024.
Values may be sent and summed in bfloat16 or wider, within the bound.
No kernel may reach another device: no remote copies, remote signals or barrier semaphores. Data moves between devices by JAX's collectives and lax.ppermute only.
A program may use at most 128 MiB of HBM per device.

```python
import math
import jax
import jax.numpy as jnp
from jax import lax

D = 4096
HEADS = 32
HEAD = 128
SEQS = 2
LENGTH = 4096
N_TENSOR = 32


def draw_tokens(key, part):
    base = jax.random.fold_in(key, 11)
    return jnp.clip(jax.random.normal(base, (SEQS, LENGTH, D), jnp.float32), -6.0, 6.0).astype(jnp.bfloat16)


def draw_w_qkv(key, part):
    base = jax.random.fold_in(key, 21)
    raw = jnp.clip(jax.random.normal(base, (D, 3, HEADS, HEAD), jnp.float32), -6.0, 6.0) / jnp.sqrt(jnp.float32(D))
    ramp = 0.6 * 3.0 ** (jnp.arange(HEADS, dtype=jnp.float32) / (HEADS - 1))
    scales = ramp * jnp.exp(jax.random.uniform(jax.random.fold_in(key, 22), (HEADS,), jnp.float32, jnp.log(0.8), jnp.log(1.25)))
    factors = jnp.stack([scales, scales, jnp.ones((HEADS,), jnp.float32)])
    raw = raw * factors[None, :, :, None]
    return jnp.clip(raw, -1.0, 1.0).reshape(D, 3, D).astype(jnp.bfloat16)


def with_spikes(values, own_key, source, target, shards_of, factor):
    def block_of(dim):
        return (jnp.arange(values.shape[dim]) // (values.shape[dim] // shards_of)).reshape((-1,) + (1,) * (values.ndim - 1 - dim))

    one_side = jax.random.permutation(own_key, shards_of)[block_of(target)]
    far = (block_of(target) + shards_of // 2) % shards_of
    return jnp.where((block_of(source) == one_side) | (block_of(source) == far), factor * values, values)


def block_levels(stream_key, extent, split, low, high):
    def one(axis_at, shards_of):
        steps = jax.random.uniform(jax.random.fold_in(jax.random.fold_in(stream_key, 6), axis_at), (shards_of,), jnp.float32, low / len(split), high / len(split))
        return jnp.repeat(jnp.exp(steps), extent[axis_at] // shards_of).reshape((-1,) + (1,) * (len(extent) - axis_at - 1))

    loudness = one(*split[0])
    for cut in split[1:]:
        loudness = loudness * one(*cut)
    return loudness


def gaussian_with(own_key, shape, scale, bound, cuts, heavy, kind=jnp.bfloat16):
    array = scale * jax.random.normal(own_key, shape, jnp.float32)
    if cuts:
        array = array * block_levels(own_key, shape, cuts, -0.22, 0.18)
    return jnp.clip(with_spikes(array, jax.random.fold_in(own_key, 3), *heavy), -bound, bound).astype(kind)


def setup_inputs(seed: int = 0) -> dict:
    splits = jax.random.split(jax.random.key(seed), 6)
    return {
        "tokens": draw_tokens(jax.random.fold_in(splits[5], 71), 0),
        "w_qkv": draw_w_qkv(jax.random.fold_in(splits[5], 71), 0),
        "q_gain": jnp.clip(jnp.exp(math.log(2.5) - 1.609438 * jax.random.uniform(splits[2], (D,), jnp.float32) ** block_levels(splits[2], (D,), ((0, 32),), -0.2, 0.2)), 0.5, 2.5),
        "k_gain": jnp.clip(jnp.exp(math.log(2.5) - 1.609438 * jax.random.uniform(splits[3], (D,), jnp.float32) ** block_levels(splits[3], (D,), ((0, 32),), -0.2, 0.2)), 0.5, 2.5),
        "w_out": gaussian_with(splits[4], (D, D), D ** -0.5, 0.1875, ((0, 32),), (0, 1, 32, 2.75)),
    }


EPS = 1e-06
ROPE_BASE = 500000.0
NEG = -1e+30

def rope_tables(positions):
    half = HEAD // 2
    freq = ROPE_BASE ** (-(jnp.arange(half, dtype=jnp.float32) * 2.0) / HEAD)
    angle = positions[:, None] * freq[None, :]
    return (jnp.cos(angle), jnp.sin(angle))

def rotate(values, cosine, sine):
    half = values.shape[-1] // 2
    first = values[..., :half]
    second = values[..., half:]
    cosine = cosine[:, None, :]
    sine = sine[:, None, :]
    return jnp.concatenate([first * cosine - second * sine, second * cosine + first * sine], -1)

def reference(tokens, w_qkv, q_gain, k_gain, w_out):
    flat = tokens.reshape(SEQS * LENGTH, D)
    query = jnp.dot(flat, w_qkv[:, 0, :], preferred_element_type=jnp.float32)
    keyed = jnp.dot(flat, w_qkv[:, 1, :], preferred_element_type=jnp.float32)
    value = jnp.dot(flat, w_qkv[:, 2, :], preferred_element_type=jnp.float32)
    inv_query = lax.rsqrt(lax.optimization_barrier(jnp.mean(query * query, -1)) + EPS)
    inv_key = lax.rsqrt(lax.optimization_barrier(jnp.mean(keyed * keyed, -1)) + EPS)
    positions = jnp.arange(LENGTH, dtype=jnp.float32)
    cosine, sine = rope_tables(positions)
    q_norm = (query * inv_query[:, None] * q_gain[None, :]).reshape(SEQS, LENGTH, HEADS, HEAD)
    k_norm = (keyed * inv_key[:, None] * k_gain[None, :]).reshape(SEQS, LENGTH, HEADS, HEAD)
    q_rot = lax.optimization_barrier(rotate(q_norm, cosine, sine).astype(jnp.bfloat16))
    k_rot = lax.optimization_barrier(rotate(k_norm, cosine, sine).astype(jnp.bfloat16))
    v_b = lax.optimization_barrier(value.astype(jnp.bfloat16)).reshape(SEQS, LENGTH, HEADS, HEAD)
    q_heads = q_rot.transpose(2, 0, 1, 3)
    k_heads = k_rot.transpose(2, 0, 1, 3)
    v_heads = v_b.transpose(2, 0, 1, 3)
    causal = jnp.arange(LENGTH)[None, :] <= jnp.arange(LENGTH)[:, None]
    scale = HEAD ** (-0.5)

    def attend(operands):
        qh, kh, vh = operands
        scores = jnp.einsum('sqd,skd->sqk', qh.astype(jnp.float32), kh.astype(jnp.float32)) * scale
        scores = jnp.where(causal[None], scores, NEG)
        top = lax.optimization_barrier(jnp.max(scores, -1))
        weights = jnp.where(causal[None], jnp.exp(scores - top[..., None]), 0.0)
        denom = lax.optimization_barrier(jnp.sum(weights, -1))
        rounded = lax.optimization_barrier(weights.astype(jnp.bfloat16)).astype(jnp.float32)
        mixed = jnp.einsum('sqk,skd->sqd', rounded, vh.astype(jnp.float32))
        return ((mixed / denom[..., None]).astype(jnp.bfloat16), jnp.max(top))
    outputs, peak = lax.map(attend, (q_heads, k_heads, v_heads))
    attended = lax.optimization_barrier(outputs.transpose(1, 2, 0, 3).reshape(SEQS * LENGTH, D))
    group = D // N_TENSOR

    def add_group(total, index):
        cols = lax.dynamic_slice_in_dim(attended, index * group, group, 1)
        rows = lax.dynamic_slice_in_dim(w_out, index * group, group, 0)
        term = lax.optimization_barrier(jnp.dot(cols, rows, preferred_element_type=jnp.float32).astype(jnp.bfloat16))
        return (total + term.astype(jnp.float32), None)
    total, unused = lax.scan(add_group, jnp.zeros((SEQS * LENGTH, D), jnp.float32), jnp.arange(N_TENSOR, dtype=jnp.int32))
    mixed = total.astype(jnp.bfloat16).reshape(SEQS, LENGTH, D)
    qk_scale = jnp.stack([inv_query, inv_key]).reshape(2, SEQS, LENGTH)
    return (mixed, peak, qk_scale)
```

```python
import jax
import jax.numpy as jnp
from jax import lax
from jax.experimental import pallas as pl
from jax.experimental.pallas import tpu as pltpu
from jax.sharding import Mesh
from jax.sharding import PartitionSpec as P


TENSOR = ("z", "y", "xh")
AXES = ("xl", "c", "z", "y", "xh")
EPS = 1e-06
ROPE_BASE = 500000.0
NEG = -1e30
LOG2E = 1.4426950408889634


ROWS = 256
QB = 512
CROSS = [(0, 3), (3, 0), (1, 2), (2, 1)]


def shift(n, k):
    return [(i, (i + k) % n) for i in range(n)]


def swap(array, axis):
    return lax.ppermute(array, axis, [(0, 1), (1, 0)])


def to_all(array, axes):
    size = lax.axis_size(axes)
    return lax.all_to_all(jnp.broadcast_to(array, (size, *array.shape[1:])), axes, 0, 0, tiled=True)


def permute(array, axis, k):
    return lax.ppermute(array, axis, shift(4, k))


def ring_direct(block, axis):
    before = permute(block, axis, 1)
    after = permute(block, axis, -1)
    far = permute(block, axis, 2)
    return before, after, far


def ring_relay(own, before, after, far, axis):
    low = jnp.stack([own, before])
    high = jnp.stack([after, far])
    before_low = permute(low, axis, 1)
    after_high = permute(high, axis, -1)
    before_high = permute(high, axis, 1)
    after_low = permute(low, axis, -1)
    far_low = permute(before_low, axis, 1)
    far_high = permute(after_high, axis, -1)
    near = (low, high, before_low, before_high, after_low, after_high)
    return near, (far_low, far_high)


def rel_slot(distance):
    d = distance % 4
    return jnp.where(d == 0, 0, jnp.where(d == 1, 2, jnp.where(d == 2, 3, 1)))


def fill_weights(idx, w_loc, w_own, w_oth, w_near, w_far):
    z, y, xh, c = idx[0], idx[1], idx[2], idx[4]

    def place(t, src, at_col, w):
        iz, iy = rel_slot(t // 8 - z), rel_slot((t // 2) % 4 - y)
        same = (t % 2) == xh
        outer = jnp.where(same, iy, iz)
        inner = jnp.where(same, iz, iy)
        base = jnp.where(same, 0, 1)
        rows = pl.ds(pl.multiple_of(src * 128, 128), 128)

        @pl.when(outer < 3)
        def _():
            to = pl.ds(pl.multiple_of((base * 12 + outer * 4 + inner) * 128, 128), 128)
            for j in range(3):
                w_near[to, at_col + 128 * j : at_col + 128 * (j + 1)] = w[j, rows, :]

        @pl.when(outer == 3)
        def _():
            to = pl.ds(pl.multiple_of((base * 4 + inner) * 128, 128), 128)
            for j in range(3):
                w_far[to, at_col + 128 * j : at_col + 128 * (j + 1)] = w[j, rows, :]

    def fill(i, carry):
        place(c * 16 + i, c * 16 + i, 0, w_loc)
        place((1 - c) * 16 + i, (1 - c) * 16 + i, 0, w_loc)
        place(c * 16 + i, i, 384, w_own)
        place((1 - c) * 16 + i, i, 384, w_oth)
        return carry

    lax.fori_loop(0, 16, fill, 0)


def near_kernel(idx, *refs):
    xs, (w_loc, w_own, w_oth, out, w_far, w_near) = refs[:12], refs[12:]

    @pl.when(pl.program_id(0) == 0)
    def _():
        fill_weights(idx, w_loc, w_own, w_oth, w_near, w_far)

    blocks = [x[i] for x in xs for i in range(2)]
    out[...] = jnp.dot(jnp.concatenate(blocks, axis=1), w_near[...], preferred_element_type=jnp.float32)


def far_kernel(idx, *refs):
    xs, (acc_ref, w_far, gains, cos_ref, sin_ref) = refs[:4], refs[4:9]
    keep_a, keep_b, send, ssq = refs[9:]
    xh, xl = idx[2], idx[3]
    step = pl.program_id(0)
    blocks = [x[i] for x in xs for i in range(2)]
    acc = acc_ref[...] + jnp.dot(
        jnp.concatenate(blocks, axis=1), w_far[...], preferred_element_type=jnp.float32
    )
    q0, k0, v0 = acc[:, :128], acc[:, 128:256], acc[:, 256:384]
    q1, k1, v1 = acc[:, 384:512], acc[:, 512:640], acc[:, 640:]
    ssq[0:1, :] = jnp.sum((q0 * q0 + q1 * q1).T, axis=0, keepdims=True)
    ssq[1:2, :] = jnp.sum((k0 * k0 + k1 * k1).T, axis=0, keepdims=True)
    cosine, sine = cos_ref[...], sin_ref[...]

    def rope(value, gain):
        value = value * gain
        return (value * cosine + pltpu.roll(value, 64, 1) * sine).astype(jnp.bfloat16)

    loc = (rope(q0, gains[0:1, :]), rope(k0, gains[1:2, :]), v0.astype(jnp.bfloat16))
    rem = (rope(q1, gains[2:3, :]), rope(k1, gains[3:4, :]), v1.astype(jnp.bfloat16))
    at = pl.multiple_of(step * ROWS, ROWS)

    def store(kept, sent):
        for i in range(3):
            send[pl.ds(pl.multiple_of(1024 * i + at, ROWS), ROWS), :] = sent[i]

        @pl.when(step < 2)
        def _():
            keep_a[pl.ds(at, ROWS), :] = kept[0]

        @pl.when(step >= 2)
        def _():
            keep_b[pl.ds(pl.multiple_of(at - 512, ROWS), ROWS), :] = kept[0]

        keep_b[pl.ds(pl.multiple_of(512 + at, ROWS), ROWS), :] = kept[1]
        keep_b[pl.ds(pl.multiple_of(1536 + at, ROWS), ROWS), :] = kept[2]

    @pl.when(xl == xh)
    def _():
        store(loc, rem)

    @pl.when(xl != xh)
    def _():
        store(rem, loc)


def whole(a):
    return pl.BlockSpec(a.shape, lambda i, s: (0,) * a.ndim)


def rows_of(a):
    return pl.BlockSpec((a.shape[0], ROWS, 128), lambda i, s: (0, i, 0))


def project_near(idx, pieces, w_loc, w_own, w_oth):
    tok = pieces[0].shape[1]
    return pl.pallas_call(
        near_kernel,
        grid_spec=pltpu.PrefetchScalarGridSpec(
            num_scalar_prefetch=1,
            grid=(tok // ROWS,),
            in_specs=[rows_of(p) for p in pieces] + [whole(w_loc), whole(w_own), whole(w_oth)],
            out_specs=(
                pl.BlockSpec((ROWS, 768), lambda i, s: (i, 0)),
                pl.BlockSpec((1024, 768), lambda i, s: (0, 0)),
            ),
            scratch_shapes=[pltpu.VMEM((3072, 768), jnp.bfloat16)],
        ),
        out_shape=(
            jax.ShapeDtypeStruct((tok, 768), jnp.float32),
            jax.ShapeDtypeStruct((1024, 768), jnp.bfloat16),
        ),
        compiler_params=pltpu.CompilerParams(
            dimension_semantics=("arbitrary",), vmem_limit_bytes=40 * 1024 * 1024
        ),
        name="project_near",
    )(idx, *pieces, w_loc, w_own, w_oth)


def project_far(idx, pieces, acc, w_far, gains, cosine, sine):
    tok = pieces[0].shape[1]
    table = pl.BlockSpec((ROWS, 128), lambda i, s: (i, 0))
    out = (
        jax.ShapeDtypeStruct((tok // 2, 128), jnp.bfloat16),
        jax.ShapeDtypeStruct((5 * tok // 2, 128), jnp.bfloat16),
        jax.ShapeDtypeStruct((3 * tok, 128), jnp.bfloat16),
        jax.ShapeDtypeStruct((2, tok), jnp.float32),
    )
    return pl.pallas_call(
        far_kernel,
        grid_spec=pltpu.PrefetchScalarGridSpec(
            num_scalar_prefetch=1,
            grid=(tok // ROWS,),
            in_specs=[rows_of(p) for p in pieces]
            + [pl.BlockSpec((ROWS, 768), lambda i, s: (i, 0))]
            + [whole(w_far), whole(gains), table, table],
            out_specs=(whole(out[0]), whole(out[1]), whole(out[2]), pl.BlockSpec((2, ROWS), lambda i, s: (0, i))),
        ),
        out_shape=out,
        compiler_params=pltpu.CompilerParams(
            dimension_semantics=("arbitrary",), vmem_limit_bytes=40 * 1024 * 1024
        ),
        name="project_far",
    )(idx, *pieces, acc, w_far, gains, cosine, sine)


def attend_kernel(idx, keep_a, keep_b, recv, d_own, d_recv, near, other, out, peak, kbuf, vbuf, qbuf, sbuf, ksbuf):
    xl, c = idx[3], idx[4]
    tok = 1024
    vbuf[:, 128:] = jnp.ones((4096, 128), jnp.bfloat16)
    pieces = (
        (xl, c, keep_a, 0, keep_b, 512, 0, near, 0),
        (1 - xl, c, recv, 0, recv, 1024, 0, near, 1),
        (xl, 1 - c, d_own, 0, d_own, 512, 512, other, 0),
        (1 - xl, 1 - c, d_recv, 0, d_recv, 512, 512, other, 1),
    )
    for lo, co, q_ref, q_at, kv_ref, k_at, half, scales, at in pieces:
        quarter = lo * 2 + co
        base = pl.multiple_of(quarter * tok, tok)
        kbuf[pl.ds(base, tok), :] = kv_ref[k_at : k_at + tok, :]
        vbuf[pl.ds(base, tok), :128] = kv_ref[k_at + tok : k_at + 2 * tok, :]
        for i in range(2):
            ksbuf[pl.ds(2 * quarter + i, 1), :] = scales[at, 1:2, QB * i : QB * (i + 1)]
        scale = scales[at, 0:1, half : half + QB] * (128 ** (-0.5) * LOG2E)
        q = q_ref[q_at : q_at + QB, :].astype(jnp.float32) * jnp.broadcast_to(scale, (128, QB)).T
        qbuf[pl.ds(pl.multiple_of(quarter * QB, QB), QB), :] = q.astype(jnp.bfloat16)

    best = jnp.full((1, 1), NEG, jnp.float32)
    row = lax.broadcasted_iota(jnp.int32, (QB, QB), 0)
    col = lax.broadcasted_iota(jnp.int32, (QB, QB), 1)
    causal = col <= row
    for quarter in range(4):
        block = 2 * quarter + jnp.where(c == quarter % 2, 0, 1)
        q = qbuf[quarter * QB : (quarter + 1) * QB, :]

        def score(j, top, masked, q=q):
            at = pl.ds(pl.multiple_of(j * QB, QB), QB)
            s = lax.dot_general(q, kbuf[at, :], (((1,), (1,)), ((), ())), preferred_element_type=jnp.float32)
            s = s * ksbuf[pl.ds(j, 1), :]
            if masked:
                s = jnp.where(causal, s, NEG)
            sbuf[j] = s
            for i in range(QB // 128):
                top = jnp.maximum(top, s[:, 128 * i : 128 * (i + 1)])
            return top

        top = score(block, jnp.full((QB, 128), NEG, jnp.float32), True)
        top = lax.fori_loop(0, block, lambda j, t: score(j, t, False), top)
        top = jnp.max(top, axis=1, keepdims=True)

        def mix(j, accum, top=top):
            at = pl.ds(pl.multiple_of(j * QB, QB), QB)
            w = jnp.exp2(sbuf[j] - top).astype(jnp.bfloat16)
            return accum + jnp.dot(w, vbuf[at, :], preferred_element_type=jnp.float32)

        accum = lax.fori_loop(0, block + 1, mix, jnp.zeros((QB, 256), jnp.float32))
        out[quarter] = (accum[:, :128] / accum[:, 128:]).astype(jnp.bfloat16)
        best = jnp.maximum(best, jnp.max(top, axis=0, keepdims=True))
    peak[...] = jnp.broadcast_to(best, peak.shape)


def attend(idx, *args):
    return pl.pallas_call(
        attend_kernel,
        grid_spec=pltpu.PrefetchScalarGridSpec(
            num_scalar_prefetch=1,
            grid=(1,),
            in_specs=[whole(a) for a in args],
            out_specs=(
                pl.BlockSpec((4, QB, 128), lambda i, s: (0, 0, 0)),
                pl.BlockSpec((8, 128), lambda i, s: (0, 0)),
            ),
            scratch_shapes=[
                pltpu.VMEM((4096, 128), jnp.bfloat16),
                pltpu.VMEM((4096, 256), jnp.bfloat16),
                pltpu.VMEM((2048, 128), jnp.bfloat16),
                pltpu.VMEM((8, QB, QB), jnp.float32),
                pltpu.VMEM((8, QB), jnp.float32),
            ],
        ),
        out_shape=(
            jax.ShapeDtypeStruct((4, QB, 128), jnp.bfloat16),
            jax.ShapeDtypeStruct((8, 128), jnp.float32),
        ),
        compiler_params=pltpu.CompilerParams(vmem_limit_bytes=50 * 1024 * 1024),
        name="attend",
    )(idx, *args)


def out_kernel(idx, x, *refs):
    mine, other, out, xbuf = refs[:4], refs[4:8], refs[8], refs[9]
    z, xh, c = idx[0], idx[2], idx[4]
    step = pl.program_id(0)

    @pl.when(step == 0)
    def _():
        for i, d in enumerate((0, 3, 1, 2)):
            zz = (z + d) % 4
            for j in range(2):
                head = xh if j == 0 else 1 - xh
                for k in range(2):
                    xbuf[128 * k : 128 * k + 128, (2 * i + j) * 128 : (2 * i + j + 1) * 128] = x[head, k, zz]

    def emit(ws):
        w = jnp.concatenate([r[j] for r in ws for j in range(2)], axis=0)
        part = jnp.dot(xbuf[...], w, preferred_element_type=jnp.float32).astype(jnp.bfloat16)
        for i in range(4):
            out[i] = part[:, 128 * i : 128 * (i + 1)]

    @pl.when(step // 4 == c)
    def _():
        emit(mine)

    @pl.when(step // 4 != c)
    def _():
        emit(other)


def out_project(idx, x, mine, other):
    def columns(which):
        return pl.BlockSpec((2, 128, 512), lambda i, s: (0, 0, jnp.clip(i - 4 * which(s[4]), 0, 3)))

    return pl.pallas_call(
        out_kernel,
        grid_spec=pltpu.PrefetchScalarGridSpec(
            num_scalar_prefetch=1,
            grid=(8,),
            in_specs=[whole(x)] + [columns(lambda c: c)] * 4 + [columns(lambda c: 1 - c)] * 4,
            out_specs=pl.BlockSpec((4, 256, 128), lambda i, s: (i, 0, 0)),
            scratch_shapes=[pltpu.VMEM((256, 1024), jnp.bfloat16)],
        ),
        out_shape=jax.ShapeDtypeStruct((32, 256, 128), jnp.bfloat16),
        compiler_params=pltpu.CompilerParams(
            dimension_semantics=("arbitrary",), vmem_limit_bytes=40 * 1024 * 1024
        ),
        name="out_project",
    )(idx, x, *mine, *other)


def rope_tables(positions, head):
    half = head // 2
    freq = ROPE_BASE ** (-(jnp.arange(half, dtype=jnp.float32) * 2.0) / head)
    angle = positions[:, None] * freq[None, :]
    cosine, sine = jnp.cos(angle), jnp.sin(angle)
    return jnp.concatenate([cosine, cosine], 1), jnp.concatenate([-sine, sine], 1)


def layer(tokens, w_qkv, q_gain, k_gain, w_out):
    seqs, tok, head = tokens.shape
    width = w_qkv.shape[0]
    half = width // 2
    xl, c, z, y, xh = (lax.axis_index(a) for a in AXES)
    idx = jnp.stack([z, y, xh, xl, c]).astype(jnp.int32)

    mine = lax.dynamic_index_in_dim(tokens, xh, 0, keepdims=False)
    theirs = swap(lax.dynamic_index_in_dim(tokens, 1 - xh, 0, keepdims=False), "xh")

    w_loc = w_qkv.transpose(1, 0, 2)
    w_own = lax.ppermute(lax.dynamic_slice_in_dim(w_loc, c * half, half, 1), ("xl", "xh"), CROSS)
    gains = jnp.stack([q_gain, k_gain])
    gains = jnp.concatenate([gains, swap(gains, "xh")], 0)

    near_a, far_a = ring_relay(mine, *ring_direct(mine, "z"), "y")
    near_b, far_b = ring_relay(theirs, *ring_direct(theirs, "y"), "z")

    w_own, *_ = lax.optimization_barrier((w_own, near_a[2], near_a[5], near_b[2], near_b[5]))
    w_oth = swap(w_own, "c")

    positions = ((xl * 2 + c) * tok + jnp.arange(tok, dtype=jnp.int32)).astype(jnp.float32)
    cosine, sine = rope_tables(positions, head)
    acc, w_near_far = project_near(idx, near_a + near_b, w_loc, w_own, w_oth)

    keep_a, keep_b, send, ssq = project_far(
        idx, (*far_a, *far_b), acc, w_near_far, gains, cosine, sine
    )

    recv = swap(send, "xl")
    d_own = swap(keep_b, "c")

    ssq = to_all(ssq[None], ("z", "y")).sum(axis=0)
    inverse = lax.rsqrt(ssq / width + EPS)

    w_half = lax.dynamic_slice_in_dim(w_out, c * half, half, 1)
    w_pair = jnp.stack([w_half, lax.ppermute(w_half, ("xl", "xh"), CROSS)])
    w_pair, inverse = lax.optimization_barrier((w_pair, inverse))
    w_before = permute(w_pair, "z", 1)
    w_after = permute(w_pair, "z", -1)
    w_far = permute(w_pair, "z", 2)

    near = jnp.stack([inverse, swap(inverse, "xl")])
    other = swap(near, "c")
    partner = swap(inverse, "xh")
    low, high = jnp.where(xh == 0, inverse, partner), jnp.where(xh == 0, partner, inverse)
    qk_scale = jnp.stack([low, high], axis=1)

    d_recv = swap(recv[tok // 2 :], "c")

    attended, top = attend(idx, keep_a, keep_b, recv, d_own, d_recv, near, other)

    attended, w_before, w_after, w_far = lax.optimization_barrier((attended, w_before, w_after, w_far))
    w_mine = (w_pair, w_before, w_after, w_far)
    w_other = tuple(swap(w, "c") for w in w_mine)

    attended = attended.reshape(16, 128, 128)
    attended = lax.all_to_all(attended, ("xl", "c", "z"), 0, 0, tiled=True)
    partial_out = out_project(idx, attended.reshape(2, 2, 4, 128, 128), w_mine, w_other)
    pieces = lax.all_to_all(partial_out, TENSOR, 0, 0, tiled=True)
    pieces = pieces.reshape(4, 4, 2, 2, 128, 128).astype(jnp.float32).sum(axis=1)
    pieces = jnp.where(c == 0, pieces, pieces[:, :, ::-1])
    mixed = pieces.transpose(1, 2, 0, 3, 4).reshape(seqs, tok, head).astype(jnp.bfloat16)
    tops = to_all(top[:1] * (1.0 / LOG2E), ("xl", "c", "xh")).reshape(2, 2, 2, 128)
    peak = lax.dynamic_index_in_dim(tops, xh, 0, keepdims=False).max(axis=(0, 1))[:1]
    return (mixed, peak, qk_scale)


def solution(mesh):
    finer = Mesh(mesh.devices.reshape(2, 2, 4, 4, 2), AXES)
    seq = ("xl", "c")
    placed = (P(None, seq, TENSOR), P(None, None, TENSOR), P(TENSOR), P(TENSOR), P(TENSOR, None))
    return jax.shard_map(
        layer,
        mesh=finer,
        in_specs=placed,
        out_specs=(P(None, seq, TENSOR), P(TENSOR), P(None, None, seq)),
        check_vma=False,
    )
```

```python
import jax
import jax.numpy as jnp
from jax import lax
from jax.experimental import pallas as pl
from jax.experimental.pallas import tpu as pltpu
from jax.sharding import Mesh
from jax.sharding import PartitionSpec as P


TENSOR = ("z", "y", "xh")
AXES = ("xl", "c", "z", "y", "xh")
EPS = 1e-06
ROPE_BASE = 500000.0
NEG = -1e30
LOG2E = 1.4426950408889634


ROWS = 256
QB = 512
OUT_COLS = 1024
OUT_STEPS = 2048 // OUT_COLS
CROSS = [(0, 3), (3, 0), (1, 2), (2, 1)]


def shift(n, k):
    return [(i, (i + k) % n) for i in range(n)]


def swap(array, axis):
    return lax.ppermute(array, axis, [(0, 1), (1, 0)])


def to_all(array, axes):
    size = lax.axis_size(axes)
    return lax.all_to_all(jnp.broadcast_to(array, (size, *array.shape[1:])), axes, 0, 0, tiled=True)


def exchange(array, axes):
    n = 2 ** len(axes)
    return lax.ppermute(array, axes, [(i, n - 1 - i) for i in range(n)])


def permute(array, axis, k):
    return lax.ppermute(array, axis, shift(4, k))


def ring_direct(block, axis):
    before = permute(block, axis, 1)
    after = permute(block, axis, -1)
    far = permute(block, axis, 2)
    return before, after, far


def ring_relay(own, before, after, far, axis):
    low = jnp.stack([own, before])
    high = jnp.stack([after, far])
    before_low = permute(low, axis, 1)
    after_high = permute(high, axis, -1)
    before_high = permute(high, axis, 1)
    after_low = permute(low, axis, -1)
    far_low = permute(before_low, axis, 1)
    far_high = permute(after_high, axis, -1)
    near = (low, high, before_low, before_high, after_low, after_high)
    return near, (far_low, far_high)


def rel_slot(distance):
    d = distance % 4
    return jnp.where(d == 0, 0, jnp.where(d == 1, 2, jnp.where(d == 2, 3, 1)))


def fill_weights(idx, w_loc, w_own, w_oth, w_near, w_far):
    z, y, xh, c = idx[0], idx[1], idx[2], idx[4]

    def place(t, src, at_col, w):
        iz, iy = rel_slot(t // 8 - z), rel_slot((t // 2) % 4 - y)
        same = (t % 2) == xh
        outer = jnp.where(same, iy, iz)
        inner = jnp.where(same, iz, iy)
        base = jnp.where(same, 0, 1)
        rows = pl.ds(pl.multiple_of(src * 128, 128), 128)

        @pl.when(outer < 3)
        def _():
            to = pl.ds(pl.multiple_of((base * 12 + outer * 4 + inner) * 128, 128), 128)
            for j in range(3):
                w_near[to, at_col + 128 * j : at_col + 128 * (j + 1)] = w[j, rows, :]

        @pl.when(outer == 3)
        def _():
            to = pl.ds(pl.multiple_of((base * 4 + inner) * 128, 128), 128)
            for j in range(3):
                w_far[to, at_col + 128 * j : at_col + 128 * (j + 1)] = w[j, rows, :]

    def fill(i, carry):
        place(c * 16 + i, c * 16 + i, 0, w_loc)
        place((1 - c) * 16 + i, (1 - c) * 16 + i, 0, w_loc)
        place(c * 16 + i, i, 384, w_own)
        place((1 - c) * 16 + i, i, 384, w_oth)
        return carry

    lax.fori_loop(0, 16, fill, 0)


def near_kernel(idx, *refs):
    xs, (w_loc, w_own, w_oth, out, w_far, w_near) = refs[:12], refs[12:]

    @pl.when(pl.program_id(0) == 0)
    def _():
        fill_weights(idx, w_loc, w_own, w_oth, w_near, w_far)

    blocks = [x[i] for x in xs for i in range(2)]
    out[...] = jnp.dot(jnp.concatenate(blocks, axis=1), w_near[...], preferred_element_type=jnp.float32)


def far_kernel(idx, *refs):
    xs, (acc_ref, w_far, gains, cos_ref, sin_ref) = refs[:4], refs[4:9]
    keep_a, keep_b, send, ssq = refs[9:]
    xh, xl = idx[2], idx[3]
    step = pl.program_id(0)
    blocks = [x[i] for x in xs for i in range(2)]
    acc = acc_ref[...] + jnp.dot(
        jnp.concatenate(blocks, axis=1), w_far[...], preferred_element_type=jnp.float32
    )
    q0, k0, v0 = acc[:, :128], acc[:, 128:256], acc[:, 256:384]
    q1, k1, v1 = acc[:, 384:512], acc[:, 512:640], acc[:, 640:]
    ssq[0:1, :] = jnp.sum((q0 * q0 + q1 * q1).T, axis=0, keepdims=True)
    ssq[1:2, :] = jnp.sum((k0 * k0 + k1 * k1).T, axis=0, keepdims=True)
    cosine, sine = cos_ref[...], sin_ref[...]

    def rope(value, gain):
        value = value * gain
        return (value * cosine + pltpu.roll(value, 64, 1) * sine).astype(jnp.bfloat16)

    loc = (rope(q0, gains[0:1, :]), rope(k0, gains[1:2, :]), v0.astype(jnp.bfloat16))
    rem = (rope(q1, gains[2:3, :]), rope(k1, gains[3:4, :]), v1.astype(jnp.bfloat16))
    at = pl.multiple_of(step * ROWS, ROWS)

    def store(kept, sent):
        for i in range(3):
            send[pl.ds(pl.multiple_of(1024 * i + at, ROWS), ROWS), :] = sent[i]

        @pl.when(step < 2)
        def _():
            keep_a[pl.ds(at, ROWS), :] = kept[0]

        @pl.when(step >= 2)
        def _():
            keep_b[pl.ds(pl.multiple_of(at - 512, ROWS), ROWS), :] = kept[0]

        keep_b[pl.ds(pl.multiple_of(512 + at, ROWS), ROWS), :] = kept[1]
        keep_b[pl.ds(pl.multiple_of(1536 + at, ROWS), ROWS), :] = kept[2]

    @pl.when(xl == xh)
    def _():
        store(loc, rem)

    @pl.when(xl != xh)
    def _():
        store(rem, loc)


def whole(a):
    return pl.BlockSpec(a.shape, lambda i, s: (0,) * a.ndim)


def rows_of(a):
    return pl.BlockSpec((a.shape[0], ROWS, 128), lambda i, s: (0, i, 0))


def project_near(idx, pieces, w_loc, w_own, w_oth):
    tok = pieces[0].shape[1]
    return pl.pallas_call(
        near_kernel,
        grid_spec=pltpu.PrefetchScalarGridSpec(
            num_scalar_prefetch=1,
            grid=(tok // ROWS,),
            in_specs=[rows_of(p) for p in pieces] + [whole(w_loc), whole(w_own), whole(w_oth)],
            out_specs=(
                pl.BlockSpec((ROWS, 768), lambda i, s: (i, 0)),
                pl.BlockSpec((1024, 768), lambda i, s: (0, 0)),
            ),
            scratch_shapes=[pltpu.VMEM((3072, 768), jnp.bfloat16)],
        ),
        out_shape=(
            jax.ShapeDtypeStruct((tok, 768), jnp.float32),
            jax.ShapeDtypeStruct((1024, 768), jnp.bfloat16),
        ),
        compiler_params=pltpu.CompilerParams(
            dimension_semantics=("arbitrary",), vmem_limit_bytes=40 * 1024 * 1024
        ),
        name="project_near",
    )(idx, *pieces, w_loc, w_own, w_oth)


def project_far(idx, pieces, acc, w_far, gains, cosine, sine):
    tok = pieces[0].shape[1]
    table = pl.BlockSpec((ROWS, 128), lambda i, s: (i, 0))
    out = (
        jax.ShapeDtypeStruct((tok // 2, 128), jnp.bfloat16),
        jax.ShapeDtypeStruct((5 * tok // 2, 128), jnp.bfloat16),
        jax.ShapeDtypeStruct((3 * tok, 128), jnp.bfloat16),
        jax.ShapeDtypeStruct((2, tok), jnp.float32),
    )
    return pl.pallas_call(
        far_kernel,
        grid_spec=pltpu.PrefetchScalarGridSpec(
            num_scalar_prefetch=1,
            grid=(tok // ROWS,),
            in_specs=[rows_of(p) for p in pieces]
            + [pl.BlockSpec((ROWS, 768), lambda i, s: (i, 0))]
            + [whole(w_far), whole(gains), table, table],
            out_specs=(whole(out[0]), whole(out[1]), whole(out[2]), pl.BlockSpec((2, ROWS), lambda i, s: (0, i))),
        ),
        out_shape=out,
        compiler_params=pltpu.CompilerParams(
            dimension_semantics=("arbitrary",), vmem_limit_bytes=40 * 1024 * 1024
        ),
        name="project_far",
    )(idx, *pieces, acc, w_far, gains, cosine, sine)


def attend_kernel(idx, keep_a, keep_b, recv, d_own, d_recv, s0, s1, s2, s3, out, peak, kbuf, vbuf, qbuf, sbuf, ksbuf):
    xl, c = idx[3], idx[4]
    tok = 1024
    vbuf[:, 128:] = jnp.ones((4096, 128), jnp.bfloat16)
    pieces = (
        (xl, c, keep_a, 0, keep_b, 512, 0, s0),
        (1 - xl, c, recv, 0, recv, 1024, 0, s1),
        (xl, 1 - c, d_own, 0, d_own, 512, 512, s2),
        (1 - xl, 1 - c, d_recv, 0, d_recv, 512, 512, s3),
    )
    for lo, co, q_ref, q_at, kv_ref, k_at, half, scales in pieces:
        quarter = lo * 2 + co
        base = pl.multiple_of(quarter * tok, tok)
        kbuf[pl.ds(base, tok), :] = kv_ref[k_at : k_at + tok, :]
        vbuf[pl.ds(base, tok), :128] = kv_ref[k_at + tok : k_at + 2 * tok, :]
        for i in range(2):
            ksbuf[pl.ds(2 * quarter + i, 1), :] = scales[1:2, QB * i : QB * (i + 1)]
        scale = scales[0:1, half : half + QB] * (128 ** (-0.5) * LOG2E)
        q = q_ref[q_at : q_at + QB, :].astype(jnp.float32) * jnp.broadcast_to(scale, (128, QB)).T
        qbuf[pl.ds(pl.multiple_of(quarter * QB, QB), QB), :] = q.astype(jnp.bfloat16)

    best = jnp.full((1, 1), NEG, jnp.float32)
    row = lax.broadcasted_iota(jnp.int32, (QB, QB), 0)
    col = lax.broadcasted_iota(jnp.int32, (QB, QB), 1)
    causal = col <= row
    for quarter in range(4):
        block = 2 * quarter + jnp.where(c == quarter % 2, 0, 1)
        q = qbuf[quarter * QB : (quarter + 1) * QB, :]

        def score(j, top, masked, q=q):
            at = pl.ds(pl.multiple_of(j * QB, QB), QB)
            s = lax.dot_general(q, kbuf[at, :], (((1,), (1,)), ((), ())), preferred_element_type=jnp.float32)
            s = s * ksbuf[pl.ds(j, 1), :]
            if masked:
                s = jnp.where(causal, s, NEG)
            sbuf[j] = s
            for i in range(QB // 128):
                top = jnp.maximum(top, s[:, 128 * i : 128 * (i + 1)])
            return top

        top = score(block, jnp.full((QB, 128), NEG, jnp.float32), True)
        top = lax.fori_loop(0, block, lambda j, t: score(j, t, False), top)
        top = jnp.max(top, axis=1, keepdims=True)

        def mix(j, accum, top=top):
            at = pl.ds(pl.multiple_of(j * QB, QB), QB)
            w = jnp.exp2(sbuf[j] - top).astype(jnp.bfloat16)
            return accum + jnp.dot(w, vbuf[at, :], preferred_element_type=jnp.float32)

        accum = lax.fori_loop(0, block + 1, mix, jnp.zeros((QB, 256), jnp.float32))
        out[quarter] = (accum[:, :128] / accum[:, 128:]).astype(jnp.bfloat16)
        best = jnp.maximum(best, jnp.max(top, axis=0, keepdims=True))
    peak[...] = jnp.broadcast_to(best, peak.shape)


def attend(idx, *args):
    return pl.pallas_call(
        attend_kernel,
        grid_spec=pltpu.PrefetchScalarGridSpec(
            num_scalar_prefetch=1,
            grid=(1,),
            in_specs=[whole(a) for a in args],
            out_specs=(
                pl.BlockSpec((4, QB, 128), lambda i, s: (0, 0, 0)),
                pl.BlockSpec((8, 128), lambda i, s: (0, 0)),
            ),
            scratch_shapes=[
                pltpu.VMEM((4096, 128), jnp.bfloat16),
                pltpu.VMEM((4096, 256), jnp.bfloat16),
                pltpu.VMEM((2048, 128), jnp.bfloat16),
                pltpu.VMEM((8, QB, QB), jnp.float32),
                pltpu.VMEM((8, QB), jnp.float32),
            ],
        ),
        out_shape=(
            jax.ShapeDtypeStruct((4, QB, 128), jnp.bfloat16),
            jax.ShapeDtypeStruct((8, 128), jnp.float32),
        ),
        compiler_params=pltpu.CompilerParams(vmem_limit_bytes=50 * 1024 * 1024),
        name="attend",
    )(idx, *args)


def out_kernel(idx, x, *refs):
    mine, other, out, xbuf = refs[:5], refs[5:10], refs[10], refs[11]
    z, xh, c = idx[0], idx[2], idx[4]
    step = pl.program_id(0)

    @pl.when(step == 0)
    def _():
        for i, d in enumerate((0, 3, 1, 2)):
            zz = (z + d) % 4
            for j in range(2):
                head = xh if j == 0 else 1 - xh
                for k in range(2):
                    xbuf[128 * k : 128 * k + 128, (2 * i + j) * 128 : (2 * i + j + 1) * 128] = x[head, k, zz]

    def emit(ws):
        acc = None
        for i in range(4):
            w = ws[i][...].reshape(256, OUT_COLS) if i < 3 else jnp.concatenate([ws[3][0], ws[4][0]], axis=0)
            part = jnp.dot(xbuf[:, 256 * i : 256 * (i + 1)], w, preferred_element_type=jnp.float32)
            acc = part if acc is None else acc + part
        acc = acc.astype(jnp.bfloat16)
        for i in range(OUT_COLS // 128):
            out[i] = acc[:, 128 * i : 128 * (i + 1)]

    @pl.when(step // OUT_STEPS == c)
    def _():
        emit(mine)

    @pl.when(step // OUT_STEPS != c)
    def _():
        emit(other)


def out_project(idx, x, mine, other):
    def columns(w, which):
        return pl.BlockSpec(
            (w.shape[0], 128, OUT_COLS),
            lambda i, s: (0, 0, jnp.clip(i - OUT_STEPS * which(s[4]), 0, OUT_STEPS - 1)),
        )

    return pl.pallas_call(
        out_kernel,
        grid_spec=pltpu.PrefetchScalarGridSpec(
            num_scalar_prefetch=1,
            grid=(2 * OUT_STEPS,),
            in_specs=[whole(x)]
            + [columns(w, lambda c: c) for w in mine]
            + [columns(w, lambda c: 1 - c) for w in other],
            out_specs=pl.BlockSpec((OUT_COLS // 128, 256, 128), lambda i, s: (i, 0, 0)),
            scratch_shapes=[pltpu.VMEM((256, 1024), jnp.bfloat16)],
        ),
        out_shape=jax.ShapeDtypeStruct((32, 256, 128), jnp.bfloat16),
        compiler_params=pltpu.CompilerParams(
            dimension_semantics=("arbitrary",), vmem_limit_bytes=40 * 1024 * 1024
        ),
        name="out_project",
    )(idx, x, *mine, *other)


def rope_tables(positions, head):
    half = head // 2
    freq = ROPE_BASE ** (-(jnp.arange(half, dtype=jnp.float32) * 2.0) / head)
    angle = positions[:, None] * freq[None, :]
    cosine, sine = jnp.cos(angle), jnp.sin(angle)
    return jnp.concatenate([cosine, cosine], 1), jnp.concatenate([-sine, sine], 1)


def layer(tokens, w_qkv, q_gain, k_gain, w_out):
    seqs, tok, head = tokens.shape
    width = w_qkv.shape[0]
    half = width // 2
    xl, c, z, y, xh = (lax.axis_index(a) for a in AXES)
    idx = jnp.stack([z, y, xh, xl, c]).astype(jnp.int32)

    mine = lax.dynamic_index_in_dim(tokens, xh, 0, keepdims=False)
    theirs = swap(lax.dynamic_index_in_dim(tokens, 1 - xh, 0, keepdims=False), "xh")

    w_loc = w_qkv.transpose(1, 0, 2)
    w_own = lax.ppermute(lax.dynamic_slice_in_dim(w_loc, c * half, half, 1), ("xl", "xh"), CROSS)
    gains = jnp.stack([q_gain, k_gain])
    gains = jnp.concatenate([gains, swap(gains, "xh")], 0)

    near_a, far_a = ring_relay(mine, *ring_direct(mine, "z"), "y")
    near_b, far_b = ring_relay(theirs, *ring_direct(theirs, "y"), "z")

    w_own, *_ = lax.optimization_barrier((w_own, near_a[2], near_a[5], near_b[2], near_b[5]))
    w_oth = swap(w_own, "c")

    positions = ((xl * 2 + c) * tok + jnp.arange(tok, dtype=jnp.int32)).astype(jnp.float32)
    cosine, sine = rope_tables(positions, head)

    w_half = lax.dynamic_slice_in_dim(w_out, c * half, half, 1)
    w_pair = jnp.stack([w_half, lax.ppermute(w_half, ("xl", "xh"), CROSS)])

    acc, w_near_far = project_near(idx, near_a + near_b, w_loc, w_own, w_oth)

    w_pair, acc = lax.optimization_barrier((w_pair, acc))
    w_before = permute(w_pair, "z", 1)
    w_after = permute(w_pair, "z", -1)

    keep_a, keep_b, send, ssq = project_far(
        idx, (*far_a, *far_b), acc, w_near_far, gains, cosine, sine
    )

    recv = swap(send, "xl")
    d_own = swap(keep_b, "c")

    ssq = to_all(ssq[None], ("z", "y")).sum(axis=0)
    inverse = lax.rsqrt(ssq / width + EPS)

    scales = (inverse, exchange(inverse, ("xl",)), exchange(inverse, ("c",)), exchange(inverse, ("xl", "c")))
    w_before, w_after, inverse = lax.optimization_barrier((w_before, w_after, inverse))
    w_far_low = permute(w_before[:1], "z", 1)
    w_far_high = permute(w_after[1:], "z", -1)

    d_recv = swap(recv[tok // 2 :], "c")

    attended, top = attend(idx, keep_a, keep_b, recv, d_own, d_recv, *scales)

    w_mine = (w_pair, w_before, w_after, w_far_low, w_far_high)
    w_other = tuple(swap(w, "c") for w in w_mine)

    attended = attended.reshape(16, 128, 128)
    attended = lax.all_to_all(attended, ("xl", "c", "z"), 0, 0, tiled=True)
    partial_out = out_project(idx, attended.reshape(2, 2, 4, 128, 128), w_mine, w_other)
    partial_out, top, inverse = lax.optimization_barrier((partial_out, top, inverse))
    pieces = lax.all_to_all(partial_out, TENSOR, 0, 0, tiled=True)
    pieces = pieces.reshape(4, 4, 2, 2, 128, 128).astype(jnp.float32).sum(axis=1)
    pieces = jnp.where(c == 0, pieces, pieces[:, :, ::-1])
    mixed = pieces.transpose(1, 2, 0, 3, 4).reshape(seqs, tok, head).astype(jnp.bfloat16)
    tops = to_all(top[:1] * (1.0 / LOG2E), ("xl", "c", "xh")).reshape(2, 2, 2, 128)
    peak = lax.dynamic_index_in_dim(tops, xh, 0, keepdims=False).max(axis=(0, 1))[:1]
    partner = swap(inverse, "xh")
    low, high = jnp.where(xh == 0, inverse, partner), jnp.where(xh == 0, partner, inverse)
    qk_scale = jnp.stack([low, high], axis=1)
    return (mixed, peak, qk_scale)


def solution(mesh):
    finer = Mesh(mesh.devices.reshape(2, 2, 4, 4, 2), AXES)
    seq = ("xl", "c")
    placed = (P(None, seq, TENSOR), P(None, None, TENSOR), P(TENSOR), P(TENSOR), P(TENSOR, None))
    return jax.shard_map(
        layer,
        mesh=finer,
        in_specs=placed,
        out_specs=(P(None, seq, TENSOR), P(TENSOR), P(None, None, seq)),
        check_vma=False,
    )
```
